32 devices in a mesh: dp: 4 (over x, core), expert: 8 (over z, y).
Axes of the slice: x: 2, y: 2, z: 4, core: 2. Of those that a mesh axis runs over, the one named last changes fastest.
Arguments:
- tokens: bfloat16 [4096, 1024], P(('dp', 'expert')), may hold values from -6 to 6
- route_a: int32 [4096, 1], P(('dp', 'expert')), may hold values from 0 to 7
- route_b: int32 [4096, 1], P(('dp', 'expert')), may hold values from 0 to 15
- gain_a: float32 [1024], replicated, may hold values from 0.25 to 1.75
- gain_b: float32 [1024], replicated, may hold values from 0.25 to 1.75
- router_a: bfloat16 [1024, 8], replicated, may hold values from -0.375 to 0.375
- router_b: bfloat16 [1024, 16], replicated, may hold values from -0.375 to 0.375
- dense_in_a: bfloat16 [1024, 4096], P(None, 'dp'), may hold values from -0.1875 to 0.1875
- dense_out_a: bfloat16 [4096, 1024], P('dp'), may hold values from -0.09375 to 0.09375
- dense_in_b: bfloat16 [1024, 4096], P(None, 'dp'), may hold values from -0.1875 to 0.1875
- dense_out_b: bfloat16 [4096, 1024], P('dp'), may hold values from -0.09375 to 0.09375
- expert_in_a: bfloat16 [8, 1024, 4096], P('expert', None, 'dp'), may hold values from -0.1875 to 0.1875
- expert_out_a: bfloat16 [8, 4096, 1024], P('expert', 'dp'), may hold values from -0.09375 to 0.09375
- expert_in_b: bfloat16 [16, 1024, 4096], P('expert', None, 'dp'), may hold values from -0.1875 to 0.1875
- expert_out_b: bfloat16 [16, 4096, 1024], P('expert', 'dp'), may hold values from -0.09375 to 0.09375
Outputs:
- stream_out: bfloat16 [4096, 1024], P(('dp', 'expert'))
The draws below stay inside these ranges and needn't reach their ends.
All inputs are finite; a program needn't handle non-finite values.
Results may differ from the reference program's by a relative error of at most 0.0091.
Values may be sent and summed in bfloat16 or wider, within the bound.
No kernel may reach another device: no remote copies, remote signals or barrier semaphores. Data moves between devices by JAX's collectives and lax.ppermute only.
A program may use at most 128 MiB of HBM per device.

```python
import jax
import jax.numpy as jnp
from jax import lax

D = 1024
FF = 4096
TOK_DEV = 128
EXPERTS_A = 8
EXPERTS_B = 16
TOKENS = 4096


def levels(own_key, dims, split, low, high):
    def one(dim, shards_of):
        heights = jax.random.uniform(jax.random.fold_in(jax.random.fold_in(own_key, 6), dim), (shards_of,), jnp.float32, low / len(split), high / len(split))
        return jnp.repeat(jnp.exp(heights), dims[dim] // shards_of).reshape((-1,) + (1,) * (len(dims) - dim - 1))

    loudness = one(*split[0])
    for cut in split[1:]:
        loudness = loudness * one(*cut)
    return loudness


def different_ones(stream_key, rows, amount, top, lift):
    order = jax.random.permutation(jax.random.fold_in(stream_key, 1), amount)
    pull = order
    for power in range(3):
        pull = pull * pull // amount
    pull = pull * lift // amount
    lots = jax.random.randint(jax.random.fold_in(stream_key, 2), (rows, amount), 0, 4096) + pull
    holders = jax.random.permutation(jax.random.fold_in(stream_key, 3), rows)[jnp.arange(amount) % rows]
    lots = jnp.where(jnp.arange(rows)[:, None] == holders[None, :], 1 << 14, lots)
    merit = lots * amount + jnp.arange(amount)
    return lax.top_k(merit.astype(jnp.int32), top)[1].astype(jnp.int32)


def gaussian(key, extent, deviation, limit, cuts=(), dtype=jnp.bfloat16):
    loudness = levels(key, extent, cuts, -0.22, 0.18) if cuts else 1.0
    array = jax.random.normal(key, extent, jnp.float32) * deviation * loudness
    return jnp.minimum(jnp.maximum(array, -limit), limit).astype(dtype)


def setup_inputs(seed: int = 0) -> dict:
    key_of = jax.random.split(jax.random.key(seed), 16)
    tokens = gaussian(key_of[0], (TOKENS, D), 1.0, 6.0, ((0, 32),))
    route_a = different_ones(key_of[1], TOKENS, EXPERTS_A, 1, 1024)
    route_b = different_ones(key_of[2], TOKENS, EXPERTS_B, 1, 512)
    gain_a = jnp.clip(1.0 + 0.15 * jax.random.normal(key_of[3], (D,), jnp.float32), 0.25, 1.75)
    gain_b = jnp.clip(1.0 + 0.15 * jax.random.normal(key_of[4], (D,), jnp.float32), 0.25, 1.75)
    router_a = gaussian(key_of[5], (D, EXPERTS_A), (D // 4) ** -0.5, 0.375)
    router_b = gaussian(key_of[6], (D, EXPERTS_B), (D // 4) ** -0.5, 0.375)
    dense_in_a = gaussian(key_of[7], (D, FF), D ** -0.5, 0.1875, ((1, 4),))
    dense_out_a = gaussian(key_of[8], (FF, D), FF ** -0.5, 0.09375, ((0, 4),))
    dense_in_b = gaussian(key_of[9], (D, FF), D ** -0.5, 0.1875, ((1, 4),))
    dense_out_b = gaussian(key_of[10], (FF, D), FF ** -0.5, 0.09375, ((0, 4),))
    expert_in_a = gaussian(key_of[11], (EXPERTS_A, D, FF), D ** -0.5, 0.1875, ((0, 8), (2, 4)))
    expert_out_a = gaussian(key_of[12], (EXPERTS_A, FF, D), FF ** -0.5, 0.09375, ((0, 8), (1, 4)))
    expert_in_b = gaussian(key_of[13], (EXPERTS_B, D, FF), D ** -0.5, 0.1875, ((0, 8), (2, 4)))
    expert_out_b = gaussian(key_of[14], (EXPERTS_B, FF, D), FF ** -0.5, 0.09375, ((0, 8), (1, 4)))
    return dict(tokens=tokens, route_a=route_a, route_b=route_b, gain_a=gain_a, gain_b=gain_b, router_a=router_a, router_b=router_b, dense_in_a=dense_in_a, dense_out_a=dense_out_a, dense_in_b=dense_in_b, dense_out_b=dense_out_b, expert_in_a=expert_in_a, expert_out_a=expert_out_a, expert_in_b=expert_in_b, expert_out_b=expert_out_b)


def norm_rows(x, gain):
    xf = x.astype(jnp.float32)
    mean = lax.optimization_barrier(jnp.mean(xf, axis=-1, keepdims=True))
    var = lax.optimization_barrier(jnp.mean((xf - mean) ** 2, axis=-1, keepdims=True))
    return ((xf - mean) / jnp.sqrt(var + 1e-05) * gain).astype(jnp.bfloat16)

def moe_layer(x, ids, gain, router, d_in, d_out, e_in, e_out):
    experts = router.shape[1]
    devices = x.shape[0] // TOK_DEV
    cap = (5 * TOK_DEV + 4 * experts - 1) // (4 * experts)
    normed = norm_rows(x, gain)
    blocks = ids.reshape(devices, TOK_DEV).astype(jnp.int32)
    onehot = (blocks[:, :, None] == jnp.arange(experts).astype(jnp.int32)[None, None, :]).astype(jnp.int32)
    before = (jnp.cumsum(onehot, axis=1) - onehot).astype(jnp.int32)
    rank = lax.optimization_barrier(jnp.sum(before * onehot, axis=-1)).astype(jnp.int32)
    kept = rank < cap
    total = devices * experts * cap
    anchor = jnp.arange(devices).astype(jnp.int32)[:, None] * (experts * cap)
    flat = jnp.where(kept, anchor + blocks * cap + rank, total).reshape(-1).astype(jnp.int32)
    logits = jnp.dot(normed, router, preferred_element_type=jnp.float32)
    picked = lax.optimization_barrier(jnp.sum(logits * onehot.reshape(-1, experts).astype(jnp.float32), axis=-1))
    gate = jax.nn.sigmoid(picked) * kept.reshape(-1).astype(jnp.float32)
    buffer = jnp.zeros((total, normed.shape[1]), jnp.bfloat16).at[flat].set(normed, mode='drop')
    buffer = buffer.reshape(devices, experts, cap, -1).transpose(1, 0, 2, 3).reshape(experts, devices * cap, -1)

    def one_expert(args):
        rows, w_first, w_second = args
        act = jax.nn.gelu(jnp.dot(rows, w_first, preferred_element_type=jnp.float32), approximate=True).astype(jnp.bfloat16)
        return jnp.dot(act, w_second, preferred_element_type=jnp.float32)
    outputs = lax.map(one_expert, (buffer, e_in, e_out))
    outputs = outputs.reshape(experts, devices, cap, -1).transpose(1, 0, 2, 3).reshape(total, -1)
    expert_tok = jnp.take(outputs, flat, axis=0, mode='fill', fill_value=0.0)

    def one_block(rows):
        act = jax.nn.gelu(jnp.dot(rows, d_in, preferred_element_type=jnp.float32), approximate=True).astype(jnp.bfloat16)
        return jnp.dot(act, d_out, preferred_element_type=jnp.float32)
    dense = lax.map(one_block, normed.reshape(devices, TOK_DEV, -1)).reshape(x.shape[0], -1)
    return (x.astype(jnp.float32) + dense + gate[:, None] * expert_tok).astype(jnp.bfloat16)

def reference(tokens, route_a, route_b, gain_a, gain_b, router_a, router_b, dense_in_a, dense_out_a, dense_in_b, dense_out_b, expert_in_a, expert_out_a, expert_in_b, expert_out_b):
    middle = moe_layer(tokens, route_a[:, 0], gain_a, router_a, dense_in_a, dense_out_a, expert_in_a, expert_out_a)
    return moe_layer(middle, route_b[:, 0], gain_b, router_b, dense_in_b, dense_out_b, expert_in_b, expert_out_b)
```

```python
import jax
import jax.numpy as jnp
from jax import lax
from jax.sharding import PartitionSpec as P


def norm_rows(x, gain):
    xf = x.astype(jnp.float32)
    mean = jnp.mean(xf, axis=-1, keepdims=True)
    var = jnp.mean((xf - mean) ** 2, axis=-1, keepdims=True)
    return ((xf - mean) / jnp.sqrt(var + 1e-05) * gain).astype(jnp.bfloat16)


def rank_table(ids, experts):
    onehot = (ids[:, None] == jnp.arange(experts)[None, :]).astype(jnp.float32)
    rows = ids.shape[0]
    earlier = (jnp.arange(rows)[:, None] > jnp.arange(rows)[None, :]).astype(jnp.float32)
    before = jnp.dot(earlier, onehot, preferred_element_type=jnp.float32)
    return onehot, jnp.sum(before * onehot, axis=-1).astype(jnp.int32)


def chip_cores(mesh):
    column = mesh.devices.reshape(mesh.shape["dp"], -1)[:, 0]
    first = tuple(column[0].coords)
    return sum(tuple(d.coords) == first for d in column)


def dp_shift(x, cores, dx, dc):
    size = lax.axis_size("dp")
    chips = size // cores
    pairs = []
    for i in range(size):
        chip, core = divmod(i, cores)
        pairs.append((i, ((chip + dx) % chips) * cores + (core + dc) % cores))
    return lax.ppermute(x, "dp", pairs)


def gather_dp(x, cores):
    chips = lax.axis_size("dp") // cores
    own = [x] + [dp_shift(x, cores, k, 0) for k in range(1, chips)]
    blocks = list(own)
    for c in range(1, cores):
        blocks += [dp_shift(b, cores, 0, c) for b in own]
    return jnp.stack(blocks)


def scatter_dp(y, cores):
    chips = lax.axis_size("dp") // cores
    y = y.reshape((cores, chips) + y.shape[1:])
    half = y[0]
    for c in range(1, cores):
        half = half + dp_shift(y[c].astype(jnp.bfloat16), cores, 0, -c).astype(jnp.float32)
    out = half[0]
    for k in range(1, chips):
        out = out + dp_shift(half[k].astype(jnp.bfloat16), cores, -k, 0).astype(jnp.float32)
    return out


def moe_layer(cores, x, ids, gain, router, d_in, d_out, e_in, e_out):
    tok_rows, width = x.shape
    experts = router.shape[1]
    owners = lax.axis_size("expert")
    per_dev = experts // owners
    cap = (5 * tok_rows + 4 * experts - 1) // (4 * experts)
    total = experts * cap
    normed = norm_rows(x, gain)
    onehot, rank = rank_table(ids, experts)
    kept = rank < cap
    slot_row = jnp.where(kept, ids * cap + rank, total)
    place = (slot_row[:, None] == jnp.arange(total)[None, :]).astype(jnp.bfloat16)

    buffer = lax.dot_general(
        place, normed, (((0,), (0,)), ((), ())), preferred_element_type=jnp.float32
    ).astype(jnp.bfloat16)
    arrived = lax.all_to_all(
        buffer.reshape(owners, per_dev, cap, width), "expert", split_axis=0, concat_axis=0, tiled=True
    )

    logits = jnp.dot(normed, router, preferred_element_type=jnp.float32)
    picked = jnp.sum(logits * onehot, axis=-1)
    gate = jax.nn.sigmoid(picked) * kept.astype(jnp.float32)

    rows = gather_dp(normed, cores)
    act = jax.nn.gelu(
        jnp.einsum("btd,df->btf", rows, d_in, preferred_element_type=jnp.float32), approximate=True
    ).astype(jnp.bfloat16)
    dense = scatter_dp(
        jnp.einsum("btf,fd->btd", act, d_out, preferred_element_type=jnp.float32), cores
    )

    rows = gather_dp(arrived, cores)
    act = jax.nn.gelu(
        jnp.einsum("bsecd,edf->bsecf", rows, e_in, preferred_element_type=jnp.float32),
        approximate=True,
    ).astype(jnp.bfloat16)
    partial = scatter_dp(
        jnp.einsum("bsecf,efd->bsecd", act, e_out, preferred_element_type=jnp.float32), cores
    )
    returned = lax.all_to_all(
        partial.astype(jnp.bfloat16), "expert", split_axis=0, concat_axis=0, tiled=True
    ).reshape(total, width)
    expert_tok = jnp.dot(place, returned, preferred_element_type=jnp.float32)
    return (x.astype(jnp.float32) + dense + gate[:, None] * expert_tok).astype(jnp.bfloat16)


def solution(mesh):
    cores = chip_cores(mesh)

    def body(
        tokens, route_a, route_b, gain_a, gain_b, router_a, router_b,
        dense_in_a, dense_out_a, dense_in_b, dense_out_b,
        expert_in_a, expert_out_a, expert_in_b, expert_out_b,
    ):
        middle = moe_layer(
            cores, tokens, route_a[:, 0], gain_a, router_a,
            dense_in_a, dense_out_a, expert_in_a, expert_out_a,
        )
        return moe_layer(
            cores, middle, route_b[:, 0], gain_b, router_b,
            dense_in_b, dense_out_b, expert_in_b, expert_out_b,
        )

    in_specs = (
        P(("dp", "expert"), None),
        P(("dp", "expert"), None),
        P(("dp", "expert"), None),
        P(),
        P(),
        P(),
        P(),
        P(None, "dp"),
        P("dp", None),
        P(None, "dp"),
        P("dp", None),
        P("expert", None, "dp"),
        P("expert", "dp", None),
        P("expert", None, "dp"),
        P("expert", "dp", None),
    )
    out_specs = P(("dp", "expert"), None)
    return jax.shard_map(body, mesh=mesh, in_specs=in_specs, out_specs=out_specs, check_vma=False)
```

```python
import jax
import jax.numpy as jnp
from jax import lax
from jax.experimental import pallas as pl
from jax.experimental.pallas import tpu as pltpu
from jax.sharding import PartitionSpec as P

VMEM_LIMIT = 48 * 1024 * 1024


def dot(a, b, lhs=1, rhs=0):
    return lax.dot_general(
        a, b, (((lhs,), (rhs,)), ((), ())), preferred_element_type=jnp.float32
    )


def chip_cores(mesh):
    column = mesh.devices.reshape(mesh.shape["dp"], -1)[:, 0]
    first = tuple(column[0].coords)
    return sum(tuple(d.coords) == first for d in column)


def dp_shift(x, cores, dx, dc):
    size = lax.axis_size("dp")
    chips = size // cores
    pairs = []
    for i in range(size):
        chip, core = divmod(i, cores)
        pairs.append((i, ((chip + dx) % chips) * cores + (core + dc) % cores))
    return lax.ppermute(x, "dp", pairs)


def front_values(xf, ids, gain, router, cap, normed_ref, buffer_ref, place_ref, gate_ref):
    rows = xf.shape[0]
    experts = router.shape[1]
    total = experts * cap
    mean = jnp.mean(xf, axis=-1, keepdims=True)
    centred = xf - mean
    var = jnp.mean(centred * centred, axis=-1, keepdims=True)
    normed = (centred * (1.0 / jnp.sqrt(var + 1e-05)) * gain).astype(jnp.bfloat16)
    normed_ref[...] = normed
    onehot = (lax.broadcasted_iota(jnp.int32, (rows, experts), 1) == ids).astype(jnp.float32)
    earlier = lax.broadcasted_iota(jnp.int32, (rows, rows), 0) > lax.broadcasted_iota(
        jnp.int32, (rows, rows), 1
    )
    before = dot(earlier.astype(jnp.float32).astype(jnp.bfloat16), onehot.astype(jnp.bfloat16))
    rank = jnp.sum(before * onehot, axis=-1, keepdims=True).astype(jnp.int32)
    kept = rank < cap
    slot = jnp.where(kept, ids * cap + rank, -1)
    place = (lax.broadcasted_iota(jnp.int32, (rows, total), 1) == slot).astype(jnp.float32)
    place = place.astype(jnp.bfloat16)
    place_ref[...] = place
    buffer_ref[...] = dot(place, normed, 0, 0).astype(jnp.bfloat16)
    logits = dot(normed, router)
    picked = jnp.sum(logits * onehot, axis=-1, keepdims=True)
    gate_ref[...] = jax.nn.sigmoid(picked) * kept.astype(jnp.float32)


def combined(x_ref, half_ref, recv_refs, place_ref, gate_ref, returned_ref):
    dense = half_ref[...]
    for r in recv_refs:
        dense = dense + r[...].astype(jnp.float32)
    expert = dot(place_ref[...], returned_ref[...])
    value = x_ref[...].astype(jnp.float32) + dense + gate_ref[...] * expert
    return value.astype(jnp.bfloat16)


def front_shapes(rows, width, total):
    return [
        jax.ShapeDtypeStruct((rows, width), jnp.bfloat16),
        jax.ShapeDtypeStruct((total, width), jnp.bfloat16),
        jax.ShapeDtypeStruct((rows, total), jnp.bfloat16),
        jax.ShapeDtypeStruct((rows, 1), jnp.float32),
    ]


def capacity(rows, experts):
    return (5 * rows + 4 * experts - 1) // (4 * experts)


def first_front(x, ids, gain, router):
    cap = capacity(x.shape[0], router.shape[1])

    def kernel(x_ref, ids_ref, gain_ref, router_ref, *outs):
        front_values(
            x_ref[...].astype(jnp.float32), ids_ref[...], gain_ref[...], router_ref[...], cap, *outs
        )

    return pl.pallas_call(
        kernel,
        out_shape=front_shapes(*x.shape, cap * router.shape[1]),
        name="first_front",
        compiler_params=pltpu.CompilerParams(vmem_limit_bytes=VMEM_LIMIT),
    )(x, ids, gain[None, :], router)


def middle_front(x, half, recvs, place, gate, returned, ids, gain, router):
    cap = capacity(x.shape[0], router.shape[1])
    n = len(recvs)

    def kernel(x_ref, half_ref, *refs):
        recv_refs, refs = refs[:n], refs[n:]
        place_ref, gate_ref, returned_ref, ids_ref, gain_ref, router_ref, x_out, *outs = refs
        value = combined(x_ref, half_ref, recv_refs, place_ref, gate_ref, returned_ref)
        x_out[...] = value
        front_values(
            value.astype(jnp.float32), ids_ref[...], gain_ref[...], router_ref[...], cap, *outs
        )

    return pl.pallas_call(
        kernel,
        out_shape=[jax.ShapeDtypeStruct(x.shape, x.dtype)]
        + front_shapes(*x.shape, cap * router.shape[1]),
        name="middle_front",
        compiler_params=pltpu.CompilerParams(vmem_limit_bytes=VMEM_LIMIT),
    )(x, half, *recvs, place, gate, returned, ids, gain[None, :], router)


def last_combine(x, half, recvs, place, gate, returned):
    n = len(recvs)

    def kernel(x_ref, half_ref, *refs):
        recv_refs, (place_ref, gate_ref, returned_ref, out_ref) = refs[:n], refs[n:]
        out_ref[...] = combined(x_ref, half_ref, recv_refs, place_ref, gate_ref, returned_ref)

    return pl.pallas_call(
        kernel,
        out_shape=jax.ShapeDtypeStruct(x.shape, x.dtype),
        name="last_combine",
        compiler_params=pltpu.CompilerParams(vmem_limit_bytes=VMEM_LIMIT),
    )(x, half, *recvs, place, gate, returned)


def feed_forward(blocks, w_in, w_out, cores, name):
    n = len(blocks)
    chips = n // cores
    per_dev, width, hidden = w_in.shape
    rows = blocks[0].shape[0] // per_dev
    tile = hidden // 4 if hidden % 1024 == 0 else hidden

    def kernel(*refs):
        block_refs = refs[:n]
        in_ref, out_w_ref, own_ref, peer_ref, row_ref, acc_ref = refs[n:]
        f = pl.program_id(1)

        @pl.when(f == 0)
        def _():
            for i, b in enumerate(block_refs):
                row_ref[i * rows : (i + 1) * rows, :] = b[...]

        act = jax.nn.gelu(dot(row_ref[...], in_ref[0]), approximate=True).astype(jnp.bfloat16)
        part = dot(act, out_w_ref[0])

        @pl.when(f == 0)
        def _():
            acc_ref[...] = part

        @pl.when(f > 0)
        def _():
            acc_ref[...] += part

        @pl.when(f == pl.num_programs(1) - 1)
        def _():
            for i in range(chips):
                own_ref[i] = acc_ref[i * rows : (i + 1) * rows, :]
            for i in range(chips, n):
                peer_ref[i - chips] = acc_ref[i * rows : (i + 1) * rows, :].astype(jnp.bfloat16)

    flops = 4 * per_dev * n * rows * width * hidden
    return pl.pallas_call(
        kernel,
        grid=(per_dev, hidden // tile),
        in_specs=[pl.BlockSpec((rows, width), lambda e, f: (e, 0))] * n
        + [
            pl.BlockSpec((1, width, tile), lambda e, f: (e, 0, f)),
            pl.BlockSpec((1, tile, width), lambda e, f: (e, f, 0)),
        ],
        out_specs=[
            pl.BlockSpec((chips, rows, width), lambda e, f: (0, e, 0)),
            pl.BlockSpec((n - chips, rows, width), lambda e, f: (0, e, 0)),
        ],
        out_shape=[
            jax.ShapeDtypeStruct((chips, per_dev * rows, width), jnp.float32),
            jax.ShapeDtypeStruct((n - chips, per_dev * rows, width), jnp.bfloat16),
        ],
        scratch_shapes=[
            pltpu.VMEM((n * rows, width), jnp.bfloat16),
            pltpu.VMEM((n * rows, width), jnp.float32),
        ],
        name=name,
        cost_estimate=pl.CostEstimate(
            flops=flops,
            transcendentals=per_dev * n * rows * hidden,
            bytes_accessed=4 * per_dev * width * hidden,
        ),
        compiler_params=pltpu.CompilerParams(vmem_limit_bytes=VMEM_LIMIT),
    )(*blocks, w_in, w_out)


def core_reduce(own, peer, cores):
    chips = own.shape[0]
    half = own
    for c in range(1, cores):
        part = dp_shift(peer[(c - 1) * chips : c * chips], cores, 0, -c)
        half = half + part.astype(jnp.float32)
    return half


def regroup(rows, outer, inner, size):
    if outer == 1 or inner == 1:
        return rows
    total = rows.shape[0]
    target = jnp.arange(total)
    i, rest = target // (outer * size), target % (outer * size)
    source = (rest // size) * (inner * size) + i * size + rest % size
    pick = (source[:, None] == jnp.arange(total)[None, :]).astype(jnp.bfloat16)
    return jnp.dot(pick, rows, preferred_element_type=jnp.float32).astype(jnp.bfloat16)


def exchange(buffer, owners):
    total, width = buffer.shape
    out = lax.all_to_all(
        buffer.reshape(owners, total // owners, width), "expert", split_axis=0, concat_axis=0, tiled=True
    )
    return out.reshape(total, width)


def blocks_over_dp(normed, buffer, cap, cores, d_in, d_out, e_in, e_out):
    chips = lax.axis_size("dp") // cores
    owners = lax.axis_size("expert")
    per_dev = e_in.shape[0]

    dense = [normed] + [dp_shift(normed, cores, k, 0) for k in range(1, chips)]
    for c in range(1, cores):
        dense = dense + [dp_shift(b, cores, 0, c) for b in dense[:chips]]

    arrived = regroup(exchange(buffer, owners), owners, per_dev, cap)
    own = [arrived] + [dp_shift(arrived, cores, k, 0) for k in range(1, chips)]

    d_own, d_peer = feed_forward(dense, d_in[None], d_out[None], cores, "dense_block")
    d_half = core_reduce(d_own, d_peer, cores)
    d_out_rows = [d_half[k].astype(jnp.bfloat16) for k in range(1, chips)]
    held = lax.optimization_barrier((own[1:], d_out_rows))
    own = own[:1] + list(held[0])
    d_recv = [dp_shift(b, cores, -k, 0) for k, b in enumerate(held[1], 1)]

    rows = list(own)
    for c in range(1, cores):
        rows += [dp_shift(b, cores, 0, c) for b in own]
    e_own, e_peer = feed_forward(rows, e_in, e_out, cores, "expert_block")
    e_half = core_reduce(e_own, e_peer, cores)
    sums = e_half[0]
    for k in range(1, chips):
        sums = sums + dp_shift(e_half[k].astype(jnp.bfloat16), cores, -k, 0).astype(jnp.float32)
    back = regroup(sums.astype(jnp.bfloat16), per_dev, owners, cap)
    return d_half[0], d_recv, exchange(back, owners)


def solution(mesh):
    cores = chip_cores(mesh)

    def body(
        tokens, route_a, route_b, gain_a, gain_b, router_a, router_b,
        dense_in_a, dense_out_a, dense_in_b, dense_out_b,
        expert_in_a, expert_out_a, expert_in_b, expert_out_b,
    ):
        rows = tokens.shape[0]
        normed, buffer, place, gate = first_front(tokens, route_a, gain_a, router_a)
        half, recvs, returned = blocks_over_dp(
            normed, buffer, capacity(rows, router_a.shape[1]), cores,
            dense_in_a, dense_out_a, expert_in_a, expert_out_a,
        )
        x, normed, buffer, place, gate = middle_front(
            tokens, half, recvs, place, gate, returned, route_b, gain_b, router_b
        )
        half, recvs, returned = blocks_over_dp(
            normed, buffer, capacity(rows, router_b.shape[1]), cores,
            dense_in_b, dense_out_b, expert_in_b, expert_out_b,
        )
        return last_combine(x, half, recvs, place, gate, returned)

    in_specs = (
        P(("dp", "expert"), None),
        P(("dp", "expert"), None),
        P(("dp", "expert"), None),
        P(),
        P(),
        P(),
        P(),
        P(None, "dp"),
        P("dp", None),
        P(None, "dp"),
        P("dp", None),
        P("expert", None, "dp"),
        P("expert", "dp", None),
        P("expert", None, "dp"),
        P("expert", "dp", None),
    )
    out_specs = P(("dp", "expert"), None)
    return jax.shard_map(body, mesh=mesh, in_specs=in_specs, out_specs=out_specs, check_vma=False)
```

```python
import jax
import jax.numpy as jnp
from jax import lax
from jax.experimental import pallas as pl
from jax.experimental.pallas import tpu as pltpu
from jax.sharding import PartitionSpec as P

VMEM_LIMIT = 8 * 1024 * 1024


def dot(a, b, lhs=1, rhs=0):
    return lax.dot_general(
        a, b, (((lhs,), (rhs,)), ((), ())), preferred_element_type=jnp.float32
    )


def chip_cores(mesh):
    column = mesh.devices.reshape(mesh.shape["dp"], -1)[:, 0]
    first = tuple(column[0].coords)
    return sum(tuple(d.coords) == first for d in column)


def dp_shift(x, cores, dx, dc):
    size = lax.axis_size("dp")
    chips = size // cores
    pairs = []
    for i in range(size):
        chip, core = divmod(i, cores)
        pairs.append((i, ((chip + dx) % chips) * cores + (core + dc) % cores))
    return lax.ppermute(x, "dp", pairs)


def capacity(rows, experts):
    return (5 * rows + 4 * experts - 1) // (4 * experts)


def padded(rows):
    return -(-rows // 8) * 8


def column(row):
    wide = jnp.broadcast_to(row.astype(jnp.float32), (8, row.shape[1]))
    return jnp.transpose(wide)[:, :1]


def iota(shape, dim):
    return lax.broadcasted_iota(jnp.int32, shape, dim)


def front_values(xf, ids, gain, router_t, cap, refs):
    normed_ref, buffer_ref, place_ref, gate_ref = refs
    rows = xf.shape[0]
    experts = router_t.shape[0]
    total = experts * cap
    owners, chunk = buffer_ref.shape[:2]
    stride = padded(chunk)
    mean = jnp.mean(xf, axis=-1, keepdims=True)
    centred = xf - mean
    var = jnp.mean(centred * centred, axis=-1, keepdims=True)
    normed = (centred * (1.0 / jnp.sqrt(var + 1e-05)) * gain).astype(jnp.bfloat16)
    normed_ref[...] = normed
    ids = column(ids).astype(jnp.int32)
    onehot = (iota((rows, experts), 1) == ids).astype(jnp.float32)
    earlier = iota((rows, rows), 0) > iota((rows, rows), 1)
    before = dot(earlier.astype(jnp.float32).astype(jnp.bfloat16), onehot.astype(jnp.bfloat16))
    rank = jnp.sum(before * onehot, axis=-1, keepdims=True).astype(jnp.int32)
    kept = rank < cap
    slot = jnp.where(kept, ids * cap + rank, -1)
    place = (iota((rows, total), 1) == slot).astype(jnp.float32).astype(jnp.bfloat16)
    place_ref[...] = place
    per_dev = experts // owners
    owner = jnp.floor((ids.astype(jnp.float32) + 0.5) / per_dev).astype(jnp.int32)
    wide = jnp.where(kept, slot + owner * (stride - chunk), -1)
    spread = (iota((rows, owners * stride), 1) == wide).astype(jnp.float32).astype(jnp.bfloat16)
    packed = dot(spread, normed, 0, 0)
    for o in range(owners):
        buffer_ref[o] = packed[o * stride : o * stride + chunk].astype(jnp.bfloat16)
    logits = dot(normed, router_t, 1, 1)
    picked = jnp.sum(logits * onehot, axis=-1, keepdims=True)
    gate_ref[...] = jax.nn.sigmoid(picked) * kept.astype(jnp.float32)


def combined(x_ref, own_ref, core_refs, recv_refs, place_ref, gate_ref, returned_ref):
    dense = own_ref[...]
    for r in core_refs:
        dense = dense + r[0].astype(jnp.float32)
    for r in recv_refs:
        dense = dense + r[...].astype(jnp.float32)
    expert = dot(place_ref[...], returned_ref[...])
    value = x_ref[...].astype(jnp.float32) + dense + gate_ref[...] * expert
    return value.astype(jnp.bfloat16)


def front_shapes(rows, width, cap, experts, owners):
    return [
        jax.ShapeDtypeStruct((rows, width), jnp.bfloat16),
        jax.ShapeDtypeStruct((owners, experts // owners * cap, width), jnp.bfloat16),
        jax.ShapeDtypeStruct((rows, experts * cap), jnp.bfloat16),
        jax.ShapeDtypeStruct((rows, 1), jnp.float32),
    ]


def first_front(x, ids, gain, router, owners):
    experts = router.shape[1]
    cap = capacity(x.shape[0], experts)
    args = (x, ids.reshape(1, -1), gain[None, :], router.T)

    def kernel(*refs):
        given, outs, kept, sems = refs[:4], refs[4:8], refs[8:12], refs[12]
        copies = [pltpu.make_async_copy(g, k, sems.at[i]) for i, (g, k) in enumerate(zip(given, kept))]
        for c in copies:
            c.start()
        for c in copies:
            c.wait()
        x_ref, ids_ref, gain_ref, router_ref = kept
        front_values(
            x_ref[...].astype(jnp.float32), ids_ref[...], gain_ref[...], router_ref[...], cap, outs
        )

    return pl.pallas_call(
        kernel,
        in_specs=[pl.BlockSpec(memory_space=pltpu.HBM)] * 4,
        out_shape=front_shapes(*x.shape, cap, experts, owners),
        scratch_shapes=[pltpu.VMEM(a.shape, a.dtype) for a in args]
        + [pltpu.SemaphoreType.DMA((4,))],
        name="first_front",
        compiler_params=pltpu.CompilerParams(vmem_limit_bytes=VMEM_LIMIT),
    )(*args)


def middle_front(x, dense, place, gate, returned, ids, gain, router, owners):
    experts = router.shape[1]
    cap = capacity(x.shape[0], experts)
    own, cores, recvs = dense
    nc, n = len(cores), len(recvs)

    def kernel(x_ref, own_ref, *refs):
        core_refs, recv_refs, refs = refs[:nc], refs[nc : nc + n], refs[nc + n :]
        place_ref, gate_ref, returned_ref, ids_ref, gain_ref, router_ref, x_out, *outs = refs
        value = combined(x_ref, own_ref, core_refs, recv_refs, place_ref, gate_ref, returned_ref)
        x_out[...] = value
        front_values(
            value.astype(jnp.float32), ids_ref[...], gain_ref[...], router_ref[...], cap, outs
        )

    return pl.pallas_call(
        kernel,
        out_shape=[jax.ShapeDtypeStruct(x.shape, x.dtype)]
        + front_shapes(*x.shape, cap, experts, owners),
        name="middle_front",
        compiler_params=pltpu.CompilerParams(vmem_limit_bytes=VMEM_LIMIT),
    )(x, own, *cores, *recvs, place, gate, returned, ids.reshape(1, -1), gain[None, :], router.T)


def last_combine(x, dense, place, gate, returned):
    own, cores, recvs = dense
    nc, n = len(cores), len(recvs)

    def kernel(x_ref, own_ref, *refs):
        core_refs, recv_refs, refs = refs[:nc], refs[nc : nc + n], refs[nc + n :]
        place_ref, gate_ref, returned_ref, out_ref = refs
        out_ref[...] = combined(
            x_ref, own_ref, core_refs, recv_refs, place_ref, gate_ref, returned_ref
        )

    return pl.pallas_call(
        kernel,
        out_shape=jax.ShapeDtypeStruct(x.shape, x.dtype),
        name="last_combine",
        compiler_params=pltpu.CompilerParams(vmem_limit_bytes=VMEM_LIMIT),
    )(x, own, *cores, *recvs, place, gate, returned)


def hidden_rows(blocks, w_in):
    rows = jnp.concatenate(blocks, axis=1)
    act = jnp.einsum("erd,edf->erf", rows, w_in, preferred_element_type=jnp.float32)
    act = jax.nn.gelu(act, approximate=True).astype(jnp.bfloat16)
    return lax.optimization_barrier(act)


def out_rows(act, w_out):
    return jnp.einsum("erf,efd->erd", act, w_out, preferred_element_type=jnp.float32)


def feed_forward(own, peer, w_in, w_out):
    act = hidden_rows(own + peer, w_in)
    cut = sum(b.shape[1] for b in own)
    peer_out = out_rows(act[:, cut:], w_out).astype(jnp.bfloat16)
    own_out = out_rows(act[:, :cut], w_out)
    return own_out, peer_out


def pack(own, parts, owners, cap):
    per_dev, rows, width = own.shape
    chunk = per_dev * cap
    stride = padded(chunk)
    n = len(parts)

    def kernel(own_ref, *refs):
        part_refs, out_ref = refs[:n], refs[n]
        values = []
        for e in range(per_dev):
            value = own_ref[e]
            for p in part_refs:
                value = value + p[e].astype(jnp.float32)
            values.append(value.astype(jnp.bfloat16))
        shape = (owners * stride, rows)
        target = iota(shape, 0).astype(jnp.float32)
        owner = jnp.floor((target + 0.5) / stride)
        within = target - owner * stride
        packed = 0.0
        for e in range(per_dev):
            place = within - e * cap
            source = jnp.where((place >= 0) & (place < cap), owner * cap + place, -1.0)
            pick = (iota(shape, 1).astype(jnp.float32) == source).astype(jnp.float32)
            packed = packed + dot(pick.astype(jnp.bfloat16), values[e])
        for o in range(owners):
            out_ref[o] = packed[o * stride : o * stride + chunk].astype(jnp.bfloat16)

    return pl.pallas_call(
        kernel,
        out_shape=jax.ShapeDtypeStruct((owners, chunk, width), jnp.bfloat16),
        name="pack",
        compiler_params=pltpu.CompilerParams(vmem_limit_bytes=VMEM_LIMIT),
    )(own, *parts)


def regroup(rows, owners, per_dev, cap):
    width = rows.shape[-1]
    total = owners * per_dev * cap
    rows = rows.reshape(total, width)
    if per_dev > 1:
        e, rest = jnp.arange(total) // (owners * cap), jnp.arange(total) % (owners * cap)
        source = (rest // cap) * (per_dev * cap) + e * cap + rest % cap
        pick = (source[:, None] == jnp.arange(total)[None, :]).astype(jnp.bfloat16)
        rows = jnp.dot(pick, rows, preferred_element_type=jnp.float32).astype(jnp.bfloat16)
    return rows.reshape(per_dev, owners * cap, width)


def exchange(buffer):
    return lax.all_to_all(buffer, "expert", split_axis=0, concat_axis=0, tiled=True)


def layer(normed, buffer, cap, cores, d_in, d_out, e_in, e_out):
    chips = lax.axis_size("dp") // cores
    owners = lax.axis_size("expert")
    per_dev = e_in.shape[0]
    over_x = lambda x, k: dp_shift(x, cores, k, 0)
    over_cores = lambda x, c: dp_shift(x, cores, 0, c)

    across = [over_x(normed, k) for k in range(1, chips)]
    arrived = exchange(buffer)
    peers = [over_cores(normed, c) for c in range(1, cores)]
    peers_x = [[over_cores(b, c) for b in across] for c in range(1, cores)]
    own = [b[None] for b in [normed] + across]
    peer = [b[None] for c in range(cores - 1) for b in [peers[c]] + peers_x[c]]
    d_own, d_peer = feed_forward(own, peer, d_in[None], d_out[None])
    shape = (chips,) + normed.shape
    d_own, d_peer = d_own.reshape(shape), d_peer.reshape((cores - 1,) + shape)
    d_core = [over_cores(d_peer[c - 1], -c) for c in range(1, cores)]
    d_send = d_own[1:]
    for part in d_core:
        d_send = d_send + part[1:].astype(jnp.float32)
    d_send = d_send.astype(jnp.bfloat16)

    mine = regroup(arrived, owners, per_dev, cap)
    far = [over_x(mine, k) for k in range(1, chips)]
    near_peer = [over_cores(mine, c) for c in range(1, cores)]
    n_own, n_peer = feed_forward([mine], near_peer, e_in, e_out)
    n_core = [over_cores(n_peer[:, r0 : r0 + mine.shape[1]], -c)
              for c, r0 in ((c, (c - 1) * mine.shape[1]) for c in range(1, cores))]
    far, n_own, d_send = lax.optimization_barrier((far, n_own, d_send))
    far_peer = [over_cores(b, c) for c in range(1, cores) for b in far]
    f_own, f_peer = feed_forward(far, far_peer, e_in, e_out)
    rows = f_own.shape[1]
    for c in range(1, cores):
        f_own = f_own + over_cores(f_peer[:, (c - 1) * rows : c * rows], -c).astype(jnp.float32)
    f_send = f_own.astype(jnp.bfloat16)
    step = mine.shape[1]
    f_recv = [over_x(f_send[:, (k - 1) * step : k * step], -k) for k in range(1, chips)]
    back = pack(n_own, n_core + f_recv, owners, cap)
    returned = exchange(back)
    d_recv = [over_x(d_send[k - 1], -k) for k in range(1, chips)]
    return (d_own[0], d_core, d_recv), returned.reshape(owners * per_dev * cap, -1)


def solution(mesh):
    cores = chip_cores(mesh)

    def body(
        tokens, route_a, route_b, gain_a, gain_b, router_a, router_b,
        dense_in_a, dense_out_a, dense_in_b, dense_out_b,
        expert_in_a, expert_out_a, expert_in_b, expert_out_b,
    ):
        rows = tokens.shape[0]
        owners = mesh.shape["expert"]
        normed, buffer, place, gate = first_front(tokens, route_a, gain_a, router_a, owners)
        dense, returned = layer(
            normed, buffer, capacity(rows, router_a.shape[1]), cores,
            dense_in_a, dense_out_a, expert_in_a, expert_out_a,
        )
        x, normed, buffer, place, gate = middle_front(
            tokens, dense, place, gate, returned, route_b, gain_b, router_b, owners
        )
        dense, returned = layer(
            normed, buffer, capacity(rows, router_b.shape[1]), cores,
            dense_in_b, dense_out_b, expert_in_b, expert_out_b,
        )
        return last_combine(x, dense, place, gate, returned)

    in_specs = (
        P(("dp", "expert"), None),
        P(("dp", "expert"), None),
        P(("dp", "expert"), None),
        P(),
        P(),
        P(),
        P(),
        P(None, "dp"),
        P("dp", None),
        P(None, "dp"),
        P("dp", None),
        P("expert", None, "dp"),
        P("expert", "dp", None),
        P("expert", None, "dp"),
        P("expert", "dp", None),
    )
    out_specs = P(("dp", "expert"), None)
    return jax.shard_map(body, mesh=mesh, in_specs=in_specs, out_specs=out_specs, check_vma=False)
```
